16 devices in a mesh: dp: 4 (over y, z, core), tp: 4 (over x).
Axes of the slice: x: 4, y: 2, z: 1, core: 2. Of those that a mesh axis runs over, the one named last changes fastest.
The devices are a block of a 4x4x4 slice.
Arguments:
- x: bfloat16 [256, 2560], P('dp'), parts along dimension 0
- k_cache: bfloat16 [256, 4096, 8, 128], P('dp', None, 'tp'), parts along dimension 0
- v_cache: bfloat16 [256, 4096, 8, 128], P('dp', None, 'tp'), parts along dimension 0
- gain_a: bfloat16 [2560], replicated
- wq: bfloat16 [2560, 4096], P(None, 'tp')
- wo: bfloat16 [4096, 2560], P('tp')
- gain_m: bfloat16 [2560], replicated
- w_gate: bfloat16 [2560, 9728], P(None, 'tp')
- w_up: bfloat16 [2560, 9728], P(None, 'tp')
- w_down: bfloat16 [9728, 2560], P('tp')
Outputs:
- output: bfloat16 [256, 2560], P('dp'), parts along dimension 0
There are 4 independent parts. The reference program is written for one: setup_inputs(seed, part) draws one part's arguments, and reference() takes and returns one part's arrays. A program takes and returns all parts, laid end to end along the dimension named above; an argument that names none is the same for every part.
All inputs are finite; a program needn't handle non-finite values.
Results may differ from the reference program's by a relative error of at most 0.017.
Values are sent between devices in bfloat16 or wider.
A program may use at most 1.5 GiB of HBM per device.

```python
import jax
import jax.numpy as jnp
from jax import lax

BATCH = 64
CACHE = 4096
D = 2560
HEADS = 32
KV_HEADS = 8
HEAD = 128
FF = 9728
THETA = 10000


def setup_inputs(seed: int = 0, part: int = 0) -> dict:
    kx, kc, kw, kn, kq, ko, km, kg, ku, kd = jax.random.split(jax.random.key(seed), 10)
    kx, kc, kw = (jax.random.fold_in(k, part) for k in (kx, kc, kw))

    def weights(key, rows, columns):
        return jax.random.normal(key, (rows, columns), jnp.float32) * rows**-0.5

    drawn = {
        "x": jax.random.normal(kx, (BATCH, D), jnp.float32),
        "k_cache": 2 * jax.random.normal(kc, (BATCH, CACHE, KV_HEADS, HEAD), jnp.float32),
        "v_cache": 4 * jax.random.normal(kw, (BATCH, CACHE, KV_HEADS, HEAD), jnp.float32),
        "gain_a": 1 + 0.1 * jax.random.normal(kn, (D,), jnp.float32),
        "wq": 2 * weights(kq, D, HEADS * HEAD),
        "wo": weights(ko, HEADS * HEAD, D),
        "gain_m": 1 + 0.1 * jax.random.normal(km, (D,), jnp.float32),
        "w_gate": weights(kg, D, FF),
        "w_up": weights(ku, D, FF),
        "w_down": 2 * weights(kd, FF, D),
    }
    return {k: v.astype(jnp.bfloat16) for k, v in drawn.items()}


def normed(x, gain):
    wide = x.astype(jnp.float32)
    scale = lax.rsqrt(jnp.mean(wide * wide, -1, keepdims=True) + 1e-6)
    return (wide * scale * gain.astype(jnp.float32)).astype(jnp.bfloat16)


def turned(t, place, theta):
    half = t.shape[-1] // 2
    angle = place.astype(jnp.float32)[:, None] * theta ** (-jnp.arange(half, dtype=jnp.float32) / half)
    cos, sin = jnp.cos(angle)[:, None], jnp.sin(angle)[:, None]
    a, b = t[..., :half].astype(jnp.float32), t[..., half:].astype(jnp.float32)
    return jnp.concatenate([a * cos - b * sin, b * cos + a * sin], -1).astype(jnp.bfloat16)


def matmul(a, w):
    return jnp.dot(a, w, preferred_element_type=jnp.float32).astype(jnp.bfloat16)


def einsum(form, a, b):
    return jnp.einsum(form, a.astype(jnp.float32), b.astype(jnp.float32))


def seen_by(a, wq, k_cache, v_cache, head, theta):
    batch, cache, kv_heads = k_cache.shape[:3]
    place = jnp.full((batch,), cache - 1)
    q = turned(matmul(a, wq).reshape(batch, -1, head), place, theta).reshape(batch, kv_heads, -1, head)
    scores = einsum("bgsd,bugd->bgsu", q, k_cache) * head**-0.5
    weights = jax.nn.softmax(scores, -1).astype(jnp.bfloat16)
    return einsum("bgsu,bugd->bgsd", weights, v_cache).astype(jnp.bfloat16).reshape(batch, -1)


def hidden_of(b, w_gate, w_up):
    gate = jnp.dot(b, w_gate, preferred_element_type=jnp.float32)
    up = jnp.dot(b, w_up, preferred_element_type=jnp.float32)
    return (jax.nn.silu(gate) * up).astype(jnp.bfloat16)


def reference(x, k_cache, v_cache, gain_a, wq, wo, gain_m, w_gate, w_up, w_down):
    seen = seen_by(normed(x, gain_a), wq, k_cache, v_cache, HEAD, THETA)
    h = (x.astype(jnp.float32) + jnp.dot(seen, wo, preferred_element_type=jnp.float32)).astype(jnp.bfloat16)
    hidden = hidden_of(normed(h, gain_m), w_gate, w_up)
    return (h.astype(jnp.float32) + jnp.dot(hidden, w_down, preferred_element_type=jnp.float32)).astype(jnp.bfloat16)
```

```python
import functools

import jax
import jax.numpy as jnp
import numpy as np
from jax import lax
from jax.experimental import pallas as pl
from jax.experimental.pallas import tpu as pltpu
from jax.sharding import PartitionSpec as P

HEAD = 128
THETA = 10000
DEPTH = 4
TILE = 256
LANES = 128
MESH = pl.DeviceIdType.MESH
F32, BF16 = jnp.float32, jnp.bfloat16
EPS = 1e-6


def dot(a, b):
    return jnp.dot(a, b, preferred_element_type=F32)


def rope_rows(place, head):
    half = head // 2
    angle = place * float(THETA) ** (-np.arange(half, dtype=np.float64) / half)
    cos, sin = np.cos(angle), np.sin(angle)
    return np.stack([np.concatenate([cos, cos]), np.concatenate([-sin, sin])]).astype(np.float32)


def pieces_of(width, step):
    return [(at, min(step, width - at)) for at in range(0, width, step)]


def layer_kernel(
    n, chunks, hidden_pieces, q_pieces,
    x_hbm, k_hbm, v_hbm, gain_a_hbm, gain_m_hbm, rope_hbm, wq_hbm, wo_hbm, wg_hbm, wu_hbm, wd_hbm, out_hbm,
    x_ref, gain_a_ref, gain_m_ref, rope_ref, kbuf, vbuf, wo_ref, wg_refs, wu_refs, wd_ref,
    b_ref, q_ref, seen_ref, s_a, s_b, h_ref, hid_ref, term_refs, rs_send, rs_recv, y_ref,
    x_sem, aux_sem, k_sem, v_sem, wq_sem, wo_sem, wg_sem, wu_sem, wd_sem, out_sem,
    t_send, t_recv, r_send, r_recv, g_send, g_recv,
):
    me = lax.axis_index("tp")
    batch, d = x_ref.shape
    heads = q_ref.shape[0] // batch
    span = kbuf.shape[2]
    block = wd_ref.shape[2]
    peer = [lax.rem(me + s, n) for s in range(n)]

    def copy_k(i):
        slot = lax.rem(i, DEPTH)
        return pltpu.make_async_copy(k_hbm.at[i], kbuf.at[slot], k_sem.at[slot])

    def copy_v(i):
        slot = lax.rem(i, DEPTH)
        return pltpu.make_async_copy(v_hbm.at[i], vbuf.at[slot], v_sem.at[slot])

    copy_x = pltpu.make_async_copy(x_hbm, x_ref, x_sem)
    copies_aux = [
        pltpu.make_async_copy(a, b, aux_sem.at[j])
        for j, (a, b) in enumerate(((gain_a_hbm, gain_a_ref), (gain_m_hbm, gain_m_ref), (rope_hbm, rope_ref)))
    ]
    copy_wo = pltpu.make_async_copy(wo_hbm, wo_ref, wo_sem)
    copies_wq = [
        pltpu.make_async_copy(wq_hbm.at[:, pl.ds(at, w)], wg_refs[j], wq_sem.at[j]) for j, (at, w) in enumerate(q_pieces)
    ]
    copies_wg = [
        pltpu.make_async_copy(wg_hbm.at[:, pl.ds(at, w)], wg_refs[j], wg_sem.at[j]) for j, (at, w) in enumerate(hidden_pieces)
    ]
    copies_wu = [
        pltpu.make_async_copy(wu_hbm.at[:, pl.ds(at, w)], wu_refs[j], wu_sem.at[j]) for j, (at, w) in enumerate(hidden_pieces)
    ]
    order = [2, 1, 3, 0]
    copies_wd = [
        pltpu.make_async_copy(
            wd_hbm.at[:, pl.ds(pl.multiple_of(peer[s] * block, LANES), block)], wd_ref.at[j], wd_sem.at[j]
        )
        for j, s in enumerate(order)
    ]

    copy_x.start()
    for c in copies_aux:
        c.start()
    for c in copies_wq:
        c.start()
    barrier = pltpu.get_barrier_semaphore()
    for s in range(1, n):
        pl.semaphore_signal(barrier, inc=1, device_id={"tp": peer[s]}, device_id_type=MESH)

    def normed(wide, gain):
        scale = lax.rsqrt(jnp.mean(wide * wide, -1, keepdims=True) + EPS)
        return (wide * scale * gain).astype(BF16)

    copy_x.wait()
    for c in copies_aux:
        c.wait()
    for i in range(DEPTH):
        copy_k(i).start()
        copy_v(i).start()
    copy_wo.start()
    gain_a = gain_a_ref[...].astype(F32).reshape(1, d)
    gain_m = gain_m_ref[...].astype(F32).reshape(1, d)
    for r in range(0, batch, 16):
        b_ref[r : r + 16, :] = normed(x_ref[r : r + 16, :].astype(F32), gain_a)
    cos, sin = rope_ref[0:1, :], rope_ref[1:2, :]
    for j, (at, w) in enumerate(q_pieces):
        copies_wq[j].wait()
        part = dot(b_ref[...], wg_refs[j][...]).astype(BF16).astype(F32)
        for c in range(0, w, HEAD):
            t = part[:, c : c + HEAD]
            t = t * cos + pltpu.roll(t, HEAD // 2, 1) * sin
            q_ref[pl.ds((at + c) // HEAD, batch, stride=heads), :] = t.astype(BF16).astype(F32)

    row = lax.broadcasted_iota(jnp.int32, (2 * heads, TILE), 0)
    lane = lax.broadcasted_iota(jnp.int32, (2 * heads, TILE), 1)
    valid = (lane % 2) == ((row % heads) // (heads // 2))
    factor = HEAD**-0.5 * float(np.log2(np.e))
    tiles = range(0, span, TILE)

    def scores(i, s_ref):
        slot = lax.rem(i, DEPTH)
        q = q_ref[pl.ds(pl.multiple_of(i * heads, heads), heads), :]
        zero = jnp.zeros_like(q)
        lhs = jnp.concatenate([jnp.concatenate([q, zero], 1), jnp.concatenate([zero, q], 1)], 0).astype(BF16)
        for t in tiles:
            both = jnp.concatenate([kbuf[slot, 0, t : t + TILE, :], kbuf[slot, 1, t : t + TILE, :]], 1)
            s_ref[:, t : t + TILE] = lax.dot_general(lhs, both, (((1,), (1,)), ((), ())), preferred_element_type=F32)

    def paired(rows, op):
        both = op(rows[:heads], rows[heads:])
        return jnp.concatenate([both, both], 0)

    def attend(i, s_ref):
        slot = lax.rem(i, DEPTH)
        top = s_ref[:, :TILE]
        for t in tiles[1:]:
            top = jnp.maximum(top, s_ref[:, t : t + TILE])
        top = jnp.max(jnp.where(valid, top, -jnp.inf), 1, keepdims=True)
        top = jnp.where(valid, paired(top, jnp.maximum), jnp.inf)
        total = jnp.zeros((2 * heads, TILE), F32)
        for t in tiles:
            e = jnp.exp2((s_ref[:, t : t + TILE] - top) * factor)
            s_ref[:, t : t + TILE] = e
            total = total + e
        inverse = 1.0 / paired(jnp.sum(total, 1, keepdims=True), jnp.add)
        parts = [None, None]
        for c, t in enumerate(tiles):
            weights = (s_ref[:, t : t + TILE] * inverse).astype(BF16)
            both = jnp.concatenate([vbuf[slot, 0, t : t + TILE, :], vbuf[slot, 1, t : t + TILE, :]], 1)
            r = dot(weights, both)
            parts[c % 2] = r if parts[c % 2] is None else parts[c % 2] + r
        r = parts[0] + parts[1]
        seen_ref[pl.ds(pl.multiple_of(i * heads, heads), heads), :] = r[:heads, :HEAD] + r[heads:, HEAD:]

    def refill(copy, i):
        @pl.when(i < batch)
        def _():
            copy(i).start()

    def pair(i):
        copy_k(i + 1).wait()
        copy_v(i).wait()
        scores(i + 1, s_b)
        attend(i, s_a)
        refill(copy_v, i + DEPTH)
        refill(copy_k, i + 1 + DEPTH)
        copy_k(i + 2).wait()
        copy_v(i + 1).wait()
        scores(i + 2, s_a)
        attend(i + 1, s_b)
        refill(copy_v, i + 1 + DEPTH)
        refill(copy_k, i + 2 + DEPTH)

    def send_term(c, s):
        return pltpu.make_async_remote_copy(
            src_ref=term_refs[c].at[me], dst_ref=term_refs[c].at[me], send_sem=t_send.at[c, s - 1], recv_sem=t_recv.at[c, s - 1],
            device_id={"tp": peer[s]}, device_id_type=MESH,
        )

    def project(c, first, count):
        seen = jnp.concatenate(
            [seen_ref[pl.ds(first * heads + g, count, stride=heads), :] for g in range(heads)], 1
        ).astype(BF16)
        for at, w in pieces_of(d, 512):
            term_refs[c][me, :, at : at + w] = dot(seen, wo_ref[:, at : at + w]).astype(BF16)
        for s in (2, 1, 3):
            send_term(c, s).start()

    last_start = batch - 2 - DEPTH

    def start_weights():
        for g, u in zip(copies_wg, copies_wu):
            g.start(priority=1)
            u.start(priority=1)
        for c in copies_wd:
            c.start(priority=1)

    copy_k(0).wait()
    scores(0, s_a)
    copy_k(DEPTH).start()
    for c, (first, count) in enumerate(chunks):
        final = c == len(chunks) - 1

        @pl.loop(0, count // 2 - (1 if final else 0))
        def _(j):
            i = first + 2 * j
            pair(i)

            if final:
                @pl.when(i == last_start)
                def _():
                    start_weights()

        if final:
            i = batch - 2
            copy_k(i + 1).wait()
            copy_v(i).wait()
            scores(i + 1, s_b)
            attend(i, s_a)
            copy_v(i + 1).wait()
            attend(i + 1, s_b)
        if c == 0:
            copy_wo.wait()
            pl.semaphore_wait(barrier, n - 1)
        project(c, first, count)

    for c, (first, count) in enumerate(chunks):
        for s in range(1, n):
            send_term(c, s).wait_recv()
        for r in range(0, count, 16):
            total = term_refs[c][0, r : r + 16, :].astype(F32)
            for s in range(1, n):
                total = total + term_refs[c][s, r : r + 16, :].astype(F32)
            at = first + r
            h = (x_ref[at : at + 16, :].astype(F32) + total).astype(BF16)
            h_ref[at : at + 16, :] = h
            b_ref[at : at + 16, :] = normed(h.astype(F32), gain_m)

    for j, (at, w) in enumerate(hidden_pieces):
        copies_wg[j].wait()
        gate = dot(b_ref[...], wg_refs[j][...])
        copies_wu[j].wait()
        up = dot(b_ref[...], wu_refs[j][...])
        hid_ref[:, at : at + w] = (gate / (1.0 + jnp.exp(-gate)) * up).astype(BF16)

    def send_block(j):
        return pltpu.make_async_remote_copy(
            src_ref=rs_send.at[j], dst_ref=rs_recv.at[j], send_sem=r_send.at[j], recv_sem=r_recv.at[j],
            device_id={"tp": peer[order[j]]}, device_id_type=MESH,
        )

    for j in range(n - 1):
        copies_wd[j].wait()
        rs_send[j] = dot(hid_ref[...], wd_ref[j]).astype(BF16)
        send_block(j).start()
    copies_wd[n - 1].wait()
    total = dot(hid_ref[...], wd_ref[n - 1])
    total = total + h_ref[:, pl.ds(pl.multiple_of(me * block, LANES), block)].astype(F32)
    for j in (1, 2, 0):
        send_block(j).wait_recv()
        total = total + rs_recv[j].astype(F32)
    y_ref[me] = total.astype(BF16)

    def send_done(s):
        return pltpu.make_async_remote_copy(
            src_ref=y_ref.at[me], dst_ref=y_ref.at[me], send_sem=g_send.at[s - 1], recv_sem=g_recv.at[s - 1],
            device_id={"tp": peer[s]}, device_id_type=MESH,
        )

    def write(s):
        owner = peer[(n - s) % n]
        return pltpu.make_async_copy(
            y_ref.at[owner], out_hbm.at[:, pl.ds(pl.multiple_of(owner * block, LANES), block)], out_sem.at[s]
        )

    for s in (2, 1, 3):
        send_done(s).start()
    write(0).start()
    for s in (1, 3, 2):
        send_done(s).wait_recv()
        write(s).start()
    for c in range(len(chunks)):
        for s in range(1, n):
            send_term(c, s).wait_send()
    for j in range(n - 1):
        send_block(j).wait_send()
    for s in range(1, n):
        send_done(s).wait_send()
    for s in range(n):
        write(s).wait()


def solution(mesh):
    n = mesh.shape["tp"]

    def step(x, k_cache, v_cache, gain_a, wq, wo, gain_m, w_gate, w_up, w_down):
        batch, cache, kv_heads, head = k_cache.shape
        d = x.shape[1]
        hidden = w_gate.shape[1]
        heads = wq.shape[1] // head
        span = cache * kv_heads // 2
        k = k_cache.reshape(batch, 2, span, head)
        v = v_cache.reshape(batch, 2, span, head)
        chunks = [(0, batch // 2), (batch // 2, batch // 4), (3 * batch // 4, batch // 4)]
        hidden_pieces = pieces_of(hidden, 512)
        q_pieces = pieces_of(wq.shape[1], 512)
        block = d // n
        dma = pltpu.SemaphoreType.DMA
        any_space = pl.BlockSpec(memory_space=pl.ANY)
        scratch = [
            pltpu.VMEM((batch, d), BF16),
            pltpu.VMEM((d,), BF16),
            pltpu.VMEM((d,), BF16),
            pltpu.VMEM((2, head), F32),
            pltpu.VMEM((DEPTH, 2, span, head), BF16),
            pltpu.VMEM((DEPTH, 2, span, head), BF16),
            pltpu.VMEM(wo.shape, BF16),
            [pltpu.VMEM((d, w), BF16) for _, w in hidden_pieces],
            [pltpu.VMEM((d, w), BF16) for _, w in hidden_pieces],
            pltpu.VMEM((n, hidden, block), BF16),
            pltpu.VMEM((batch, d), BF16),
            pltpu.VMEM((batch * heads, head), F32),
            pltpu.VMEM((batch * heads, head), F32),
            pltpu.VMEM((2 * heads, span), F32),
            pltpu.VMEM((2 * heads, span), F32),
            pltpu.VMEM((batch, d), BF16),
            pltpu.VMEM((batch, hidden), BF16),
            [pltpu.VMEM((n, count, d), BF16) for _, count in chunks],
            pltpu.VMEM((n - 1, batch, block), BF16),
            pltpu.VMEM((n - 1, batch, block), BF16),
            pltpu.VMEM((n, batch, block), BF16),
            dma(()), dma((3,)), dma((DEPTH,)), dma((DEPTH,)), dma((len(q_pieces),)), dma(()),
            dma((len(hidden_pieces),)), dma((len(hidden_pieces),)), dma((n,)), dma((n,)),
            dma((len(chunks), n - 1)), dma((len(chunks), n - 1)), dma((n - 1,)), dma((n - 1,)), dma((n - 1,)), dma((n - 1,)),
        ]
        return pl.pallas_call(
            functools.partial(layer_kernel, n, chunks, hidden_pieces, q_pieces),
            out_shape=jax.ShapeDtypeStruct(x.shape, x.dtype),
            in_specs=[any_space] * 11,
            out_specs=any_space,
            scratch_shapes=scratch,
            compiler_params=pltpu.CompilerParams(collective_id=0, has_side_effects=True, vmem_limit_bytes=67043328),
            name="layer",
        )(x, k, v, gain_a, gain_m, jnp.asarray(rope_rows(cache - 1, head)), wq, wo, w_gate, w_up, w_down)

    states, cache, columns, rows_of = P("dp", None), P("dp", None, "tp", None), P(None, "tp"), P("tp", None)
    return jax.shard_map(
        step,
        mesh=mesh,
        in_specs=(states, cache, cache, P(None), columns, rows_of, P(None), columns, columns, rows_of),
        out_specs=states,
        check_vma=False,
    )
```

```python
import functools

import jax
import jax.numpy as jnp
import numpy as np
from jax import lax
from jax.experimental import pallas as pl
from jax.experimental.pallas import tpu as pltpu
from jax.sharding import PartitionSpec as P

HEAD = 128
THETA = 10000
DEPTH = 4
TILE = 256
LANES = 128
VMEM_BYTES = 67043328
MESH = pl.DeviceIdType.MESH
F32, BF16 = jnp.float32, jnp.bfloat16
EPS = 1e-6


def dot(a, b):
    return jnp.dot(a, b, preferred_element_type=F32)


def rope_rows(place, head):
    half = head // 2
    angle = place * float(THETA) ** (-np.arange(half, dtype=np.float64) / half)
    cos, sin = np.cos(angle), np.sin(angle)
    return np.stack([np.concatenate([cos, cos]), np.concatenate([-sin, sin])]).astype(np.float32)


def pieces_of(width, step):
    return [(at, min(step, width - at)) for at in range(0, width, step)]


def layer_kernel(
    n, chunks, hidden_pieces, q_pieces, out_pieces,
    x_hbm, k_hbm, v_hbm, gain_a_hbm, gain_m_hbm, rope_hbm, wq_hbm, wo_hbm, wg_hbm, wu_hbm, wd_hbm, out_hbm,
    x_ref, gain_a_ref, gain_m_ref, rope_ref, kbuf, vbuf, wo_ref, wg_refs, wu_refs, wd_refs,
    b_ref, q_ref, seen_ref, s_a, s_b, h_ref, hid_ref, term_refs, own_refs, rs_send, rs_recv, y_refs,
    x_sem, aux_sem, k_sem, v_sem, wq_sem, wo_sem, wg_sem, wu_sem, wd_sem, out_sem,
    t_send, t_recv, r_send, r_recv, g_send, g_recv,
):
    me = lax.axis_index("tp")
    batch, d = x_ref.shape
    heads = q_ref.shape[0] // batch
    span = kbuf.shape[2]
    peer = [lax.rem(me + s, n) for s in range(n)]

    def copy_k(i):
        slot = lax.rem(i, DEPTH)
        return pltpu.make_async_copy(k_hbm.at[i], kbuf.at[slot], k_sem.at[slot])

    def copy_v(i):
        slot = lax.rem(i, DEPTH)
        return pltpu.make_async_copy(v_hbm.at[i], vbuf.at[slot], v_sem.at[slot])

    copy_x = pltpu.make_async_copy(x_hbm, x_ref, x_sem)
    copies_aux = [
        pltpu.make_async_copy(a, b, aux_sem.at[j])
        for j, (a, b) in enumerate(((gain_a_hbm, gain_a_ref), (gain_m_hbm, gain_m_ref), (rope_hbm, rope_ref)))
    ]
    copy_wo = pltpu.make_async_copy(wo_hbm, wo_ref, wo_sem)
    copies_wq = [
        pltpu.make_async_copy(wq_hbm.at[:, pl.ds(at, w)], wg_refs[j], wq_sem.at[j]) for j, (at, w) in enumerate(q_pieces)
    ]
    copies_wg = [
        pltpu.make_async_copy(wg_hbm.at[:, pl.ds(at, w)], wg_refs[j], wg_sem.at[j]) for j, (at, w) in enumerate(hidden_pieces)
    ]
    copies_wu = [
        pltpu.make_async_copy(wu_hbm.at[:, pl.ds(at, w)], wu_refs[j], wu_sem.at[j]) for j, (at, w) in enumerate(hidden_pieces)
    ]
    copies_wd = [
        pltpu.make_async_copy(wd_hbm.at[:, pl.ds(at, w)], wd_refs[p], wd_sem.at[p]) for p, (at, w) in enumerate(out_pieces)
    ]

    copy_x.start()
    for c in copies_aux:
        c.start()
    for c in copies_wq:
        c.start()
    barrier = pltpu.get_barrier_semaphore()
    for s in range(1, n):
        pl.semaphore_signal(barrier, inc=1, device_id={"tp": peer[s]}, device_id_type=MESH)

    def normed(wide, gain):
        scale = lax.rsqrt(jnp.mean(wide * wide, -1, keepdims=True) + EPS)
        return (wide * scale * gain).astype(BF16)

    copy_x.wait()
    for c in copies_aux:
        c.wait()
    for i in range(DEPTH):
        copy_k(i).start()
        copy_v(i).start()
    copy_wo.start()
    gain_a = gain_a_ref[...].astype(F32).reshape(1, d)
    gain_m = gain_m_ref[...].astype(F32).reshape(1, d)
    for r in range(0, batch, 16):
        b_ref[r : r + 16, :] = normed(x_ref[r : r + 16, :].astype(F32), gain_a)
    cos, sin = rope_ref[0:1, :], rope_ref[1:2, :]
    for j, (at, w) in enumerate(q_pieces):
        copies_wq[j].wait()
        part = dot(b_ref[...], wg_refs[j][...]).astype(BF16).astype(F32)
        for c in range(0, w, HEAD):
            t = part[:, c : c + HEAD]
            t = t * cos + pltpu.roll(t, HEAD // 2, 1) * sin
            q_ref[pl.ds((at + c) // HEAD, batch, stride=heads), :] = t.astype(BF16).astype(F32)

    row = lax.broadcasted_iota(jnp.int32, (2 * heads, TILE), 0)
    lane = lax.broadcasted_iota(jnp.int32, (2 * heads, TILE), 1)
    valid = (lane % 2) == ((row % heads) // (heads // 2))
    factor = HEAD**-0.5 * float(np.log2(np.e))
    tiles = range(0, span, TILE)

    def scores(i, s_ref):
        slot = lax.rem(i, DEPTH)
        q = q_ref[pl.ds(pl.multiple_of(i * heads, heads), heads), :]
        zero = jnp.zeros_like(q)
        lhs = jnp.concatenate([jnp.concatenate([q, zero], 1), jnp.concatenate([zero, q], 1)], 0).astype(BF16)
        for t in tiles:
            both = jnp.concatenate([kbuf[slot, 0, t : t + TILE, :], kbuf[slot, 1, t : t + TILE, :]], 1)
            s_ref[:, t : t + TILE] = lax.dot_general(lhs, both, (((1,), (1,)), ((), ())), preferred_element_type=F32)

    def paired(rows, op):
        both = op(rows[:heads], rows[heads:])
        return jnp.concatenate([both, both], 0)

    def attend(i, s_ref, ready=None):
        slot = lax.rem(i, DEPTH)
        top = s_ref[:, :TILE]
        for t in tiles[1:]:
            top = jnp.maximum(top, s_ref[:, t : t + TILE])
        top = jnp.max(jnp.where(valid, top, -jnp.inf), 1, keepdims=True)
        top = jnp.where(valid, paired(top, jnp.maximum), jnp.inf)
        total = jnp.zeros((2 * heads, TILE), F32)
        for t in tiles:
            e = jnp.exp2((s_ref[:, t : t + TILE] - top) * factor)
            s_ref[:, t : t + TILE] = e
            total = total + e
        inverse = 1.0 / paired(jnp.sum(total, 1, keepdims=True), jnp.add)
        if ready is not None:
            ready.wait()
        parts = [None, None]
        for c, t in enumerate(tiles):
            weights = (s_ref[:, t : t + TILE] * inverse).astype(BF16)
            both = jnp.concatenate([vbuf[slot, 0, t : t + TILE, :], vbuf[slot, 1, t : t + TILE, :]], 1)
            r = dot(weights, both)
            parts[c % 2] = r if parts[c % 2] is None else parts[c % 2] + r
        r = parts[0] + parts[1]
        seen_ref[pl.ds(pl.multiple_of(i * heads, heads), heads), :] = r[:heads, :HEAD] + r[heads:, HEAD:]

    def refill(copy, i):
        @pl.when(i < batch)
        def _():
            copy(i).start()

    def pair(i):
        copy_k(i + 1).wait()
        copy_v(i).wait()
        scores(i + 1, s_b)
        attend(i, s_a)
        refill(copy_v, i + DEPTH)
        refill(copy_k, i + 1 + DEPTH)
        copy_k(i + 2).wait()
        copy_v(i + 1).wait()
        scores(i + 2, s_a)
        attend(i + 1, s_b)
        refill(copy_v, i + 1 + DEPTH)
        refill(copy_k, i + 2 + DEPTH)

    def landed(ref, sem):
        return pltpu.make_async_copy(ref, ref, sem)

    def send_term(c, s):
        mine = term_refs[c].at[me]
        return pltpu.make_async_remote_copy(
            src_ref=mine, dst_ref=mine, send_sem=t_send.at[c], recv_sem=t_recv.at[c],
            device_id={"tp": peer[s]}, device_id_type=MESH,
        )

    def project(c, first, count):
        seen = jnp.concatenate(
            [seen_ref[pl.ds(first * heads + g, count, stride=heads), :] for g in range(heads)], 1
        ).astype(BF16)
        for at, w in out_pieces:
            term_refs[c][me, :, at : at + w] = dot(seen, wo_ref[:, at : at + w]).astype(BF16)
        for s in (2, 1, 3):
            send_term(c, s).start()

    streamed = [c for pair_of in zip(copies_wg, copies_wu) for c in pair_of] + copies_wd

    def stream(first, count):
        for c in streamed[first : first + count]:
            c.start()

    copy_k(0).wait()
    scores(0, s_a)
    copy_k(DEPTH).start()
    for c, (first, count) in enumerate(chunks):
        final = c == len(chunks) - 1

        @pl.loop(0, count // 2 - (1 if final else 0))
        def _(j):
            i = first + 2 * j
            pair(i)

            if final:
                @pl.when(i == batch - 6)
                def _():
                    stream(0, 1)

                @pl.when(i == batch - 4)
                def _():
                    stream(1, 4)

        if final:
            i = batch - 2
            copy_k(i + 1).wait()
            copy_v(i).wait()
            scores(i + 1, s_b)
            attend(i, s_a)
            stream(5, 2)
            attend(i + 1, s_b, copy_v(i + 1))
            stream(7, 2)
        if c == 0:
            copy_wo.wait()
            pl.semaphore_wait(barrier, n - 1)
        project(c, first, count)

    ahead = len(streamed) - 9
    out_groups = [(0, 1), (2, 3, 4)]
    for j in range(ahead):
        streamed[j].wait()
        stream(9 + j, 1)

    for c, (first, count) in enumerate(chunks):
        landed(term_refs[c].at[pl.ds(0, n - 1)], t_recv.at[c]).wait()
        for r in range(0, count, 8):
            total = term_refs[c][0, r : r + 8, :].astype(F32)
            for s in range(1, n):
                total = total + term_refs[c][s, r : r + 8, :].astype(F32)
            at = first + r
            h = (x_ref[at : at + 8, :].astype(F32) + total).astype(BF16)
            h_ref[at : at + 8, :] = h
            b_ref[at : at + 8, :] = normed(h.astype(F32), gain_m)

    for start, upto in ((0, 3), (3, len(hidden_pieces))):
        for c in streamed[max(ahead, 2 * start) : 2 * upto]:
            c.wait()
        for j, (at, w) in list(enumerate(hidden_pieces))[start:upto]:
            gate = dot(b_ref[...], wg_refs[j][...])
            up = dot(b_ref[...], wu_refs[j][...])
            hid_ref[:, at : at + w] = (gate / (1.0 + jnp.exp(-gate)) * up).astype(BF16)

    def share(at, w):
        return pl.ds(pl.multiple_of(at + me * (w // n), LANES), w // n)

    def send_part(p, s):
        return pltpu.make_async_remote_copy(
            src_ref=rs_send[p].at[peer[s]], dst_ref=rs_recv[p].at[s - 1], send_sem=r_send, recv_sem=r_recv.at[p],
            device_id={"tp": peer[s]}, device_id_type=MESH,
        )

    def send_done(p, s):
        mine = y_refs[p].at[:, share(0, out_pieces[p][1])]
        return pltpu.make_async_remote_copy(
            src_ref=mine, dst_ref=mine, send_sem=g_send, recv_sem=g_recv.at[p], device_id={"tp": peer[s]}, device_id_type=MESH,
        )

    def write(p):
        at, w = out_pieces[p]
        return pltpu.make_async_copy(y_refs[p], out_hbm.at[:, pl.ds(at, w)], out_sem)

    for group in out_groups:
        for p in group:
            copies_wd[p].wait()
        for p in group:
            term = dot(hid_ref[...], wd_refs[p][...])
            own_refs[p][...] = term
            width = out_pieces[p][1] // n
            for j in range(n):
                rs_send[p][j] = term[:, j * width : (j + 1) * width].astype(BF16)
            for s in (2, 1, 3):
                send_part(p, s).start()
    for p, (at, w) in enumerate(out_pieces):
        landed(rs_recv[p], r_recv.at[p]).wait()
        total = own_refs[p][:, share(0, w)]
        for s in range(1, n):
            total = total + rs_recv[p][s - 1].astype(F32)
        y_refs[p][:, share(0, w)] = (h_ref[:, share(at, w)].astype(F32) + total).astype(BF16)
        for s in (2, 1, 3):
            send_done(p, s).start()
    for p, (at, w) in enumerate(out_pieces):
        landed(y_refs[p].at[:, pl.ds(0, w - w // n)], g_recv.at[p]).wait()
        write(p).start()
    for c in range(len(chunks)):
        landed(term_refs[c].at[pl.ds(0, n - 1)], t_send.at[c]).wait()
    for sem in (r_send, g_send):
        landed(h_ref.at[:, pl.ds(0, d - d // n)], sem).wait()
    landed(h_ref, out_sem).wait()


def solution(mesh):
    n = mesh.shape["tp"]

    def step(x, k_cache, v_cache, gain_a, wq, wo, gain_m, w_gate, w_up, w_down):
        batch, cache, kv_heads, head = k_cache.shape
        d = x.shape[1]
        hidden = w_gate.shape[1]
        heads = wq.shape[1] // head
        span = cache * kv_heads // 2
        k = k_cache.reshape(batch, 2, span, head)
        v = v_cache.reshape(batch, 2, span, head)
        last = 8
        chunks = [(0, batch // 2), (batch // 2, batch // 2 - last), (batch - last, last)]
        hidden_pieces = pieces_of(hidden, 512)
        q_pieces = pieces_of(wq.shape[1], 512)
        out_pieces = pieces_of(d, 512)
        dma = pltpu.SemaphoreType.DMA
        any_space = pl.BlockSpec(memory_space=pl.ANY)
        scratch = [
            pltpu.VMEM((batch, d), BF16),
            pltpu.VMEM((d,), BF16),
            pltpu.VMEM((d,), BF16),
            pltpu.VMEM((2, head), F32),
            pltpu.VMEM((DEPTH, 2, span, head), BF16),
            pltpu.VMEM((DEPTH, 2, span, head), BF16),
            pltpu.VMEM(wo.shape, BF16),
            [pltpu.VMEM((d, w), BF16) for _, w in hidden_pieces],
            [pltpu.VMEM((d, w), BF16) for _, w in hidden_pieces],
            [pltpu.VMEM((hidden, w), BF16) for _, w in out_pieces],
            pltpu.VMEM((batch, d), BF16),
            pltpu.VMEM((batch * heads, head), F32),
            pltpu.VMEM((batch * heads, head), F32),
            pltpu.VMEM((2 * heads, span), F32),
            pltpu.VMEM((2 * heads, span), F32),
            pltpu.VMEM((batch, d), BF16),
            pltpu.VMEM((batch, hidden), BF16),
            [pltpu.VMEM((n, count, d), BF16) for _, count in chunks],
            [pltpu.VMEM((batch, w), F32) for _, w in out_pieces],
            [pltpu.VMEM((n, batch, w // n), BF16) for _, w in out_pieces],
            [pltpu.VMEM((n - 1, batch, w // n), BF16) for _, w in out_pieces],
            [pltpu.VMEM((batch, w), BF16) for _, w in out_pieces],
            dma(()), dma((3,)), dma((DEPTH,)), dma((DEPTH,)), dma((len(q_pieces),)), dma(()),
            dma((len(hidden_pieces),)), dma((len(hidden_pieces),)), dma((len(out_pieces),)), dma(()),
            dma((len(chunks),)), dma((len(chunks),)),
            dma(()), dma((len(out_pieces),)), dma(()), dma((len(out_pieces),)),
        ]
        return pl.pallas_call(
            functools.partial(layer_kernel, n, chunks, hidden_pieces, q_pieces, out_pieces),
            out_shape=jax.ShapeDtypeStruct(x.shape, x.dtype),
            in_specs=[any_space] * 11,
            out_specs=any_space,
            scratch_shapes=scratch,
            compiler_params=pltpu.CompilerParams(collective_id=0, has_side_effects=True, vmem_limit_bytes=VMEM_BYTES),
            name="layer",
        )(x, k, v, gain_a, gain_m, jnp.asarray(rope_rows(cache - 1, head)), wq, wo, w_gate, w_up, w_down)

    states, cache, columns, rows_of = P("dp", None), P("dp", None, "tp", None), P(None, "tp"), P("tp", None)
    return jax.shard_map(
        step,
        mesh=mesh,
        in_specs=(states, cache, cache, P(None), columns, rows_of, P(None), columns, columns, rows_of),
        out_specs=states,
        check_vma=False,
    )
```

```python
import functools

import jax
import jax.numpy as jnp
import numpy as np
from jax import lax
from jax.experimental import pallas as pl
from jax.experimental.pallas import tpu as pltpu
from jax.sharding import PartitionSpec as P

HEAD = 128
THETA = 10000
DEPTH = 4
TILE = 256
LANES = 128
VMEM_BYTES = 67043328
MESH = pl.DeviceIdType.MESH
F32, BF16 = jnp.float32, jnp.bfloat16
EPS = 1e-6
STEPS = (((0, 1, 2), ()), ((3, 4), (0,)), ((), (1, 2)), ((), (3, 4)))


def dot(a, b):
    return jnp.dot(a, b, preferred_element_type=F32)


def rope_rows(place, head):
    half = head // 2
    angle = place * float(THETA) ** (-np.arange(half, dtype=np.float64) / half)
    cos, sin = np.cos(angle), np.sin(angle)
    return np.stack([np.concatenate([cos, cos]), np.concatenate([-sin, sin])]).astype(np.float32)


def pieces_of(width, step):
    return [(at, min(step, width - at)) for at in range(0, width, step)]


def layer_kernel(
    n, chunks, hidden_pieces, q_pieces, out_pieces,
    x_hbm, k_hbm, v_hbm, gain_a_hbm, gain_m_hbm, rope_hbm, wq_hbm, wo_hbm, wg_hbm, wu_hbm, wd_hbm, out_hbm,
    x_ref, gain_a_ref, gain_m_ref, rope_ref, kbuf, vbuf, wo_ref, wg_refs, wu_refs, wd_refs,
    b_ref, q_ref, seen_ref, s_a, s_b, h_ref, hid_ref, term_refs, own_refs, rs_send, rs_recv, y_refs,
    x_sem, aux_sem, k_sem, v_sem, wq_sem, wo_sem, wg_sem, wu_sem, wd_sem, out_sem,
    t_send, t_recv, r_send, r_recv, g_send, g_recv,
):
    me = lax.axis_index("tp")
    batch, d = x_ref.shape
    heads = q_ref.shape[0] // batch
    span = kbuf.shape[2]
    peer = [lax.rem(me + s, n) for s in range(n)]

    def copy_k(i):
        slot = lax.rem(i, DEPTH)
        return pltpu.make_async_copy(k_hbm.at[i], kbuf.at[slot], k_sem.at[slot])

    def copy_v(i):
        slot = lax.rem(i, DEPTH)
        return pltpu.make_async_copy(v_hbm.at[i], vbuf.at[slot], v_sem.at[slot])

    copy_x = pltpu.make_async_copy(x_hbm, x_ref, x_sem)
    copies_aux = [
        pltpu.make_async_copy(a, b, aux_sem.at[j])
        for j, (a, b) in enumerate(((gain_a_hbm, gain_a_ref), (gain_m_hbm, gain_m_ref), (rope_hbm, rope_ref)))
    ]
    copy_wo = pltpu.make_async_copy(wo_hbm, wo_ref, wo_sem)
    copies_wq = [
        pltpu.make_async_copy(wq_hbm.at[:, pl.ds(at, w)], wg_refs[j], wq_sem.at[j]) for j, (at, w) in enumerate(q_pieces)
    ]
    copies_wg = [
        pltpu.make_async_copy(wg_hbm.at[:, pl.ds(at, w)], wg_refs[j], wg_sem.at[j]) for j, (at, w) in enumerate(hidden_pieces)
    ]
    copies_wu = [
        pltpu.make_async_copy(wu_hbm.at[:, pl.ds(at, w)], wu_refs[j], wu_sem.at[j]) for j, (at, w) in enumerate(hidden_pieces)
    ]
    copies_wd = [
        pltpu.make_async_copy(wd_hbm.at[:, pl.ds(at, w)], wd_refs[p], wd_sem.at[p]) for p, (at, w) in enumerate(out_pieces)
    ]

    copy_x.start()
    for c in copies_aux:
        c.start()
    for c in copies_wq:
        c.start()
    barrier = pltpu.get_barrier_semaphore()
    for s in range(1, n):
        pl.semaphore_signal(barrier, inc=1, device_id={"tp": peer[s]}, device_id_type=MESH)

    def normed(wide, gain):
        scale = lax.rsqrt(jnp.mean(wide * wide, -1, keepdims=True) + EPS)
        return (wide * scale * gain).astype(BF16)

    copy_x.wait()
    for c in copies_aux:
        c.wait()
    for i in range(DEPTH):
        copy_k(i).start()
        copy_v(i).start()
    copy_wo.start()
    gain_a = gain_a_ref[...].astype(F32).reshape(1, d)
    gain_m = gain_m_ref[...].astype(F32).reshape(1, d)
    for r in range(0, batch, 16):
        b_ref[r : r + 16, :] = normed(x_ref[r : r + 16, :].astype(F32), gain_a)
    cos, sin = rope_ref[0:1, :], rope_ref[1:2, :]
    for j, (at, w) in enumerate(q_pieces):
        copies_wq[j].wait()
        part = dot(b_ref[...], wg_refs[j][...]).astype(BF16).astype(F32)
        for c in range(0, w, HEAD):
            t = part[:, c : c + HEAD]
            t = t * cos + pltpu.roll(t, HEAD // 2, 1) * sin
            q_ref[pl.ds((at + c) // HEAD, batch, stride=heads), :] = t.astype(BF16).astype(F32)

    row = lax.broadcasted_iota(jnp.int32, (2 * heads, TILE), 0)
    lane = lax.broadcasted_iota(jnp.int32, (2 * heads, TILE), 1)
    valid = (lane % 2) == ((row % heads) // (heads // 2))
    factor = HEAD**-0.5 * float(np.log2(np.e))
    tiles = range(0, span, TILE)

    def scores(i, s_ref):
        slot = lax.rem(i, DEPTH)
        q = q_ref[pl.ds(pl.multiple_of(i * heads, heads), heads), :]
        zero = jnp.zeros_like(q)
        lhs = jnp.concatenate([jnp.concatenate([q, zero], 1), jnp.concatenate([zero, q], 1)], 0).astype(BF16)
        for t in tiles:
            both = jnp.concatenate([kbuf[slot, 0, t : t + TILE, :], kbuf[slot, 1, t : t + TILE, :]], 1)
            s_ref[:, t : t + TILE] = lax.dot_general(lhs, both, (((1,), (1,)), ((), ())), preferred_element_type=F32)

    def paired(rows, op):
        both = op(rows[:heads], rows[heads:])
        return jnp.concatenate([both, both], 0)

    def attend(i, s_ref, ready=None):
        slot = lax.rem(i, DEPTH)
        top = s_ref[:, :TILE]
        for t in tiles[1:]:
            top = jnp.maximum(top, s_ref[:, t : t + TILE])
        top = jnp.max(jnp.where(valid, top, -jnp.inf), 1, keepdims=True)
        top = jnp.where(valid, paired(top, jnp.maximum), jnp.inf)
        total = jnp.zeros((2 * heads, TILE), F32)
        for t in tiles:
            e = jnp.exp2((s_ref[:, t : t + TILE] - top) * factor)
            s_ref[:, t : t + TILE] = e
            total = total + e
        inverse = 1.0 / paired(jnp.sum(total, 1, keepdims=True), jnp.add)
        if ready is not None:
            ready.wait()
        parts = [None, None]
        for c, t in enumerate(tiles):
            weights = (s_ref[:, t : t + TILE] * inverse).astype(BF16)
            both = jnp.concatenate([vbuf[slot, 0, t : t + TILE, :], vbuf[slot, 1, t : t + TILE, :]], 1)
            r = dot(weights, both)
            parts[c % 2] = r if parts[c % 2] is None else parts[c % 2] + r
        r = parts[0] + parts[1]
        seen_ref[pl.ds(pl.multiple_of(i * heads, heads), heads), :] = r[:heads, :HEAD] + r[heads:, HEAD:]

    def refill(copy, i):
        @pl.when(i < batch)
        def _():
            copy(i).start()

    def pair(i):
        copy_k(i + 1).wait()
        copy_v(i).wait()
        scores(i + 1, s_b)
        attend(i, s_a)
        refill(copy_v, i + DEPTH)
        refill(copy_k, i + 1 + DEPTH)
        copy_k(i + 2).wait()
        copy_v(i + 1).wait()
        scores(i + 2, s_a)
        attend(i + 1, s_b)
        refill(copy_v, i + 1 + DEPTH)
        refill(copy_k, i + 2 + DEPTH)

    def landed(ref, sem):
        return pltpu.make_async_copy(ref, ref, sem)

    def send_term(c, s):
        mine = term_refs[c].at[me]
        return pltpu.make_async_remote_copy(
            src_ref=mine, dst_ref=mine, send_sem=t_send.at[c], recv_sem=t_recv.at[c],
            device_id={"tp": peer[s]}, device_id_type=MESH,
        )

    def project(c, first, count):
        seen = jnp.concatenate(
            [seen_ref[pl.ds(first * heads + g, count, stride=heads), :] for g in range(heads)], 1
        ).astype(BF16)
        for at, w in out_pieces:
            term_refs[c][me, :, at : at + w] = dot(seen, wo_ref[:, at : at + w]).astype(BF16)
        for s in (2, 1, 3):
            send_term(c, s).start()

    streamed = [c for pair_of in zip(copies_wg, copies_wu) for c in pair_of] + copies_wd

    def stream(first, count):
        for c in streamed[first : first + count]:
            c.start()

    copy_k(0).wait()
    scores(0, s_a)
    copy_k(DEPTH).start()
    for c, (first, count) in enumerate(chunks):
        final = c == len(chunks) - 1

        @pl.loop(0, count // 2 - (1 if final else 0))
        def _(j):
            i = first + 2 * j
            pair(i)

            if final:
                @pl.when(i == batch - 6)
                def _():
                    stream(0, 1)

                @pl.when(i == batch - 4)
                def _():
                    stream(1, 4)

        if final:
            i = batch - 2
            copy_k(i + 1).wait()
            copy_v(i).wait()
            scores(i + 1, s_b)
            attend(i, s_a)
            stream(5, 2)
            attend(i + 1, s_b, copy_v(i + 1))
            stream(7, 2)
        if c == 0:
            copy_wo.wait()
            pl.semaphore_wait(barrier, n - 1)
        project(c, first, count)

    ahead = len(streamed) - 9
    for j in range(ahead):
        streamed[j].wait()
        stream(9 + j, 1)

    for c, (first, count) in enumerate(chunks):
        landed(term_refs[c].at[pl.ds(0, n - 1)], t_recv.at[c]).wait()
        for r in range(0, count, 8):
            total = term_refs[c][0, r : r + 8, :].astype(F32)
            for s in range(1, n):
                total = total + term_refs[c][s, r : r + 8, :].astype(F32)
            at = first + r
            h = (x_ref[at : at + 8, :].astype(F32) + total).astype(BF16)
            h_ref[at : at + 8, :] = h
            b_ref[at : at + 8, :] = normed(h.astype(F32), gain_m)

    def share(at, w):
        return pl.ds(pl.multiple_of(at + me * (w // n), LANES), w // n)

    def send_part(p, s):
        return pltpu.make_async_remote_copy(
            src_ref=rs_send[p].at[peer[s]], dst_ref=rs_recv[p].at[s - 1], send_sem=r_send, recv_sem=r_recv.at[p],
            device_id={"tp": peer[s]}, device_id_type=MESH,
        )

    def send_done(p, s):
        mine = y_refs[p].at[:, share(0, out_pieces[p][1])]
        return pltpu.make_async_remote_copy(
            src_ref=mine, dst_ref=mine, send_sem=g_send, recv_sem=g_recv.at[p], device_id={"tp": peer[s]}, device_id_type=MESH,
        )

    def write(p):
        at, w = out_pieces[p]
        return pltpu.make_async_copy(y_refs[p], out_hbm.at[:, pl.ds(at, w)], out_sem)

    arrived = ahead
    for inner, outer in STEPS:
        upto = 2 * len(hidden_pieces) + outer[-1] + 1 if outer else 2 * inner[-1] + 2
        for c in streamed[arrived:upto]:
            c.wait()
        arrived = max(arrived, upto)
        for j in inner:
            at, w = hidden_pieces[j]
            gate = dot(b_ref[...], wg_refs[j][...])
            up = dot(b_ref[...], wu_refs[j][...])
            hid_ref[:, at : at + w] = (gate / (1.0 + jnp.exp(-gate)) * up).astype(BF16)
        for p in outer:
            term = dot(hid_ref[...], wd_refs[p][...])
            own_refs[p][...] = term
            width = out_pieces[p][1] // n
            for j in range(n):
                rs_send[p][j] = term[:, j * width : (j + 1) * width].astype(BF16)
            for s in (2, 1, 3):
                send_part(p, s).start()
    for p, (at, w) in enumerate(out_pieces):
        landed(rs_recv[p], r_recv.at[p]).wait()
        total = own_refs[p][:, share(0, w)]
        for s in range(1, n):
            total = total + rs_recv[p][s - 1].astype(F32)
        y_refs[p][:, share(0, w)] = (h_ref[:, share(at, w)].astype(F32) + total).astype(BF16)
        for s in (2, 1, 3):
            send_done(p, s).start()
    for p, (at, w) in enumerate(out_pieces):
        landed(y_refs[p].at[:, pl.ds(0, w - w // n)], g_recv.at[p]).wait()
        write(p).start()
    for c in range(len(chunks)):
        landed(term_refs[c].at[pl.ds(0, n - 1)], t_send.at[c]).wait()
    for sem in (r_send, g_send):
        landed(h_ref.at[:, pl.ds(0, d - d // n)], sem).wait()
    landed(h_ref, out_sem).wait()


def solution(mesh):
    n = mesh.shape["tp"]

    def step(x, k_cache, v_cache, gain_a, wq, wo, gain_m, w_gate, w_up, w_down):
        batch, cache, kv_heads, head = k_cache.shape
        d = x.shape[1]
        hidden = w_gate.shape[1]
        heads = wq.shape[1] // head
        span = cache * kv_heads // 2
        k = k_cache.reshape(batch, 2, span, head)
        v = v_cache.reshape(batch, 2, span, head)
        last = 8
        chunks = [(0, batch // 2), (batch // 2, batch // 2 - last), (batch - last, last)]
        hidden_pieces = pieces_of(hidden, 512)
        q_pieces = pieces_of(wq.shape[1], 512)
        out_pieces = pieces_of(d, 512)
        dma = pltpu.SemaphoreType.DMA
        any_space = pl.BlockSpec(memory_space=pl.ANY)
        scratch = [
            pltpu.VMEM((batch, d), BF16),
            pltpu.VMEM((d,), BF16),
            pltpu.VMEM((d,), BF16),
            pltpu.VMEM((2, head), F32),
            pltpu.VMEM((DEPTH, 2, span, head), BF16),
            pltpu.VMEM((DEPTH, 2, span, head), BF16),
            pltpu.VMEM(wo.shape, BF16),
            [pltpu.VMEM((d, w), BF16) for _, w in hidden_pieces],
            [pltpu.VMEM((d, w), BF16) for _, w in hidden_pieces],
            [pltpu.VMEM((hidden, w), BF16) for _, w in out_pieces],
            pltpu.VMEM((batch, d), BF16),
            pltpu.VMEM((batch * heads, head), F32),
            pltpu.VMEM((batch * heads, head), F32),
            pltpu.VMEM((2 * heads, span), F32),
            pltpu.VMEM((2 * heads, span), F32),
            pltpu.VMEM((batch, d), BF16),
            pltpu.VMEM((batch, hidden), BF16),
            [pltpu.VMEM((n, count, d), BF16) for _, count in chunks],
            [pltpu.VMEM((batch, w), F32) for _, w in out_pieces],
            [pltpu.VMEM((n, batch, w // n), BF16) for _, w in out_pieces],
            [pltpu.VMEM((n - 1, batch, w // n), BF16) for _, w in out_pieces],
            [pltpu.VMEM((batch, w), BF16) for _, w in out_pieces],
            dma(()), dma((3,)), dma((DEPTH,)), dma((DEPTH,)), dma((len(q_pieces),)), dma(()),
            dma((len(hidden_pieces),)), dma((len(hidden_pieces),)), dma((len(out_pieces),)), dma(()),
            dma((len(chunks),)), dma((len(chunks),)),
            dma(()), dma((len(out_pieces),)), dma(()), dma((len(out_pieces),)),
        ]
        return pl.pallas_call(
            functools.partial(layer_kernel, n, chunks, hidden_pieces, q_pieces, out_pieces),
            out_shape=jax.ShapeDtypeStruct(x.shape, x.dtype),
            in_specs=[any_space] * 11,
            out_specs=any_space,
            scratch_shapes=scratch,
            compiler_params=pltpu.CompilerParams(collective_id=0, has_side_effects=True, vmem_limit_bytes=VMEM_BYTES),
            name="layer",
        )(x, k, v, gain_a, gain_m, jnp.asarray(rope_rows(cache - 1, head)), wq, wo, w_gate, w_up, w_down)

    states, cache, columns, rows_of = P("dp", None), P("dp", None, "tp", None), P(None, "tp"), P("tp", None)
    return jax.shard_map(
        step,
        mesh=mesh,
        in_specs=(states, cache, cache, P(None), columns, rows_of, P(None), columns, columns, rows_of),
        out_specs=states,
        check_vma=False,
    )
```
